32 devices in a mesh: rep: 4 (over x, core), shard: 8 (over z, y).
Axes of the slice: x: 2, y: 2, z: 4, core: 2. Of those that a mesh axis runs over, the one named last changes fastest.
Arguments:
- outer_delta: float32 [4, 2097152], P('rep', 'shard'), may hold values from -40 to 40
- offsets: int32 [65], replicated, may hold values from 0 to 2097152, as said below
- parameters: float32 [2097152], P('shard'), may hold values from -6 to 6
- momentum: float32 [2097152], P(('shard', 'rep')), may hold values from -1.2 to 1.2
Outputs:
- new_parameters: float32 [2097152], P('shard')
- new_momentum: float32 [2097152], P(('shard', 'rep'))
The draws below stay inside these ranges and needn't reach their ends.
Inputs may be any that keep to these rules, and one draw needn't show every extreme that they name: `offsets`: strictly increasing multiples of 128, the first 0 and the last 2097152.
All inputs are finite; a program needn't handle non-finite values.
Results may differ from the reference program's by a relative error of at most 0.0003.
Values sent between devices are 32-bit elements; how exact they have to be, the bound alone decides.
A program may use at most 64 MiB of HBM per device.

```python
import jax
import jax.numpy as jnp
from jax import lax

TENSORS = 64
PARAMS = 2097152
REPLICAS = 4


def tensor_bounds(key):
    slots = PARAMS // 128
    shuffled = jax.random.permutation(jax.random.fold_in(key, 11), slots - 1) + 1
    inner = jnp.sort(shuffled[:TENSORS - 1]) * 128
    first = jnp.zeros((1,), jnp.int32)
    final = jnp.full((1,), PARAMS, jnp.int32)
    return jnp.concatenate([first, inner.astype(jnp.int32), final]).astype(jnp.int32)


def draw_offsets(key, part):
    return tensor_bounds(key)


def draw_outer_delta(key, part):
    bounds = tensor_bounds(key)
    positions = jnp.arange(PARAMS, dtype=jnp.int32)
    segment = jnp.searchsorted(bounds, positions, side='right') - 1
    log_scale = jax.random.uniform(jax.random.fold_in(key, 12), (TENSORS,), jnp.float32, jnp.log(0.05), jnp.log(0.5))
    tensor_scale = jnp.exp(log_scale)
    ramp = 1.0 + 2.0 * positions.astype(jnp.float32) / PARAMS
    rep_scale = 1.0 + 2.0 * jnp.arange(REPLICAS, dtype=jnp.float32) / max(REPLICAS - 1, 1)
    noise = jnp.clip(jax.random.normal(jax.random.fold_in(key, 13), (REPLICAS, PARAMS), jnp.float32), -5.0, 5.0)
    return (noise * rep_scale[:, None] * (tensor_scale[segment] * ramp)[None, :]).astype(jnp.float32)


def steps_of(stream_key, shape, pieces, smallest, high):
    factor_of, own = 1.0, jax.random.fold_in(stream_key, 6)
    for axis_at, blocks in pieces:
        heights = jnp.exp(jax.random.uniform(jax.random.fold_in(own, axis_at), (blocks,), jnp.float32, smallest / len(pieces), high / len(pieces)))
        factor_of = factor_of * jnp.repeat(heights, shape[axis_at] // blocks).reshape([-1 if axis == axis_at else 1 for axis in range(len(shape))])
    return factor_of


def bell_draw(key, dims, scale, most, shards=(), kind=jnp.bfloat16):
    result = jax.random.normal(key, dims, jnp.float32) * scale
    if len(shards) > 0:
        result = steps_of(key, dims, shards, -0.22, 0.18) * result
    return jnp.clip(result, min=-most, max=most).astype(kind)


def setup_inputs(seed: int = 0) -> dict:
    streams_of = jax.random.split(jax.random.key(seed), 5)
    return {
        "outer_delta": draw_outer_delta(jax.random.fold_in(streams_of[4], 71), 0),
        "offsets": draw_offsets(jax.random.fold_in(streams_of[4], 71), 0),
        "parameters": bell_draw(streams_of[2], (PARAMS,), 1.0, 6.0, ((0, 8),), jnp.float32),
        "momentum": bell_draw(streams_of[3], (PARAMS,), 0.2, 1.2, ((0, 32),), jnp.float32),
    }


LR_OUTER = 0.7
MU_OUTER = 0.9
CLIP_RMS = 0.1
EPSILON = 1e-06

def reference(outer_delta, offsets, parameters, momentum):
    avg_delta = lax.optimization_barrier(jnp.sum(outer_delta, axis=0)) / jnp.float32(REPLICAS)
    positions = jnp.arange(PARAMS, dtype=jnp.int32)
    segment = (jnp.searchsorted(offsets, positions, side='right') - 1).astype(jnp.int32)
    squares_sum = jax.ops.segment_sum(avg_delta * avg_delta, segment, num_segments=TENSORS)
    lengths = (offsets[1:] - offsets[:-1]).astype(jnp.float32)
    factor = jnp.minimum(1.0, CLIP_RMS * jnp.sqrt(lengths) * lax.rsqrt(squares_sum + EPSILON))
    scaled = avg_delta * factor[segment]
    new_momentum = MU_OUTER * momentum + scaled
    new_parameters = parameters - LR_OUTER * (scaled + MU_OUTER * new_momentum)
    return (new_parameters, new_momentum)
```

```python
import functools

import jax
import jax.numpy as jnp
from jax import lax
from jax.experimental import pallas as pl
from jax.experimental.pallas import tpu as pltpu
from jax.sharding import PartitionSpec as P

LR_OUTER = 0.7
MU_OUTER = 0.9
CLIP_RMS = 0.1
EPSILON = 1e-06
LANES = 128
MESH = pl.DeviceIdType.MESH


def split_dot(wide):
    high = wide.astype(jnp.bfloat16)
    low = (wide - high.astype(jnp.float32)).astype(jnp.bfloat16)
    both = jnp.concatenate([high, low], axis=1)
    ones = jnp.ones((2 * LANES, LANES), jnp.bfloat16)
    return jnp.dot(both, ones, preferred_element_type=jnp.float32)


def outer_step(
    replicas, shards, tensors, block, chunk,
    offsets, delta_in, params_in, momentum_in,
    full, new_momentum,
    delta, params, momentum, from_twin, chip_sum, from_chips, average, partial, partials,
    load_sem, twin_send, twin_recv, chip_send, chip_recv, norm_send, norm_recv,
    out_send, out_recv, own_send, own_recv, pass_send, pass_recv,
):
    chips = replicas // 2
    pieces = block // chunk
    devices = replicas * shards
    rep = lax.axis_index("rep")
    shard = lax.axis_index("shard")
    me = rep * shards + shard
    chip = lax.div(rep, 2)
    core = lax.rem(rep, 2)
    twin = (rep + 1) - 2 * core

    def chip_at(step):
        return lax.rem(chip + step, chips)

    def part(piece):
        return pl.ds(piece * chunk, chunk)

    own_rows = pl.ds(pl.multiple_of(rep * block, 8), block)
    loads = [
        pltpu.make_async_copy(delta_in, delta, load_sem.at[0]),
        pltpu.make_async_copy(params_in.at[own_rows], params, load_sem.at[1]),
        pltpu.make_async_copy(momentum_in, momentum, load_sem.at[2]),
    ]
    for load in loads:
        load.start()

    barrier = pltpu.get_barrier_semaphore()

    def greet(step, carry):
        other = lax.rem(me + step, devices)
        pl.semaphore_signal(
            barrier, inc=1, device_id=(lax.div(other, shards), lax.rem(other, shards)),
            device_id_type=MESH,
        )
        return carry

    lax.fori_loop(1, devices, greet, 0)

    lane = lax.broadcasted_iota(jnp.int32, (1, LANES), 1)
    first = jnp.zeros((1, LANES), jnp.int32)
    last = jnp.zeros((1, LANES), jnp.int32)
    for t in range(tensors):
        first = jnp.where(lane == t, offsets[t], first)
        last = jnp.where(lane == t, offsets[t + 1], last)

    loads[0].wait()
    pl.semaphore_wait(barrier, devices - 1)

    def block_rows(owner, piece):
        return pl.ds(pl.multiple_of(owner * block + piece * chunk, 8), chunk)

    steps = list(range(1, chips)) + [0]
    twin_copies = {}
    for step in steps:
        for piece in range(pieces):
            owner = 2 * chip_at(step) + (1 - core)
            copy = pltpu.make_async_remote_copy(
                src_ref=delta.at[block_rows(owner, piece)],
                dst_ref=from_twin.at[step, part(piece)],
                send_sem=twin_send.at[step, piece],
                recv_sem=twin_recv.at[step, piece],
                device_id=(twin, shard),
                device_id_type=MESH,
            )
            copy.start()
            twin_copies[step, piece] = copy

    chip_copies = {}
    for piece in range(pieces):
        for step in range(1, chips):
            owner = 2 * chip_at(step) + core
            twin_copies[step, piece].wait_recv()
            chip_sum[step - 1, part(piece)] = (
                delta[block_rows(owner, piece)] + from_twin[step, part(piece)]
            )
            copy = pltpu.make_async_remote_copy(
                src_ref=chip_sum.at[step - 1, part(piece)],
                dst_ref=from_chips.at[step - 1, part(piece)],
                send_sem=chip_send.at[step - 1, piece],
                recv_sem=chip_recv.at[step - 1, piece],
                device_id=(owner, shard),
                device_id_type=MESH,
            )
            copy.start()
            chip_copies[step, piece] = copy

    base = (shard * replicas + rep) * block

    def in_tensor(piece):
        row = lax.broadcasted_iota(jnp.int32, (chunk, LANES), 0)
        position = (row + (base + piece * chunk)) * LANES
        return (position >= first) & (position < last)

    squares = jnp.zeros((1, LANES), jnp.float32)
    for piece in range(pieces):
        twin_copies[0, piece].wait_recv()
        total = delta[block_rows(rep, piece)] + from_twin[0, part(piece)]
        for step in range(1, chips):
            chip_copies[step, piece].wait_recv()
            total = total + from_chips[step - 1, part(piece)]
        mean = total * jnp.float32(1.0 / replicas)
        average[part(piece)] = mean
        row_sums = split_dot(mean * mean)
        squares = squares + jnp.sum(
            jnp.where(in_tensor(piece), row_sums, 0.0), axis=0, keepdims=True
        )
    partial[...] = squares

    def tell(step, carry):
        other = lax.rem(me + step, devices)
        pltpu.make_async_remote_copy(
            src_ref=partial,
            dst_ref=partials.at[pl.ds(step - 1, 1)],
            send_sem=norm_send,
            recv_sem=norm_recv,
            device_id=(lax.div(other, shards), lax.rem(other, shards)),
            device_id_type=MESH,
        ).start()
        return carry

    lax.fori_loop(1, devices, tell, 0)
    loads[1].wait()
    loads[2].wait()
    pltpu.make_async_copy(partials, partials, norm_recv).wait()
    squares = squares + jnp.sum(partials[...], axis=0, keepdims=True)
    lengths = (last - first).astype(jnp.float32)
    factor = jnp.minimum(1.0, CLIP_RMS * jnp.sqrt(lengths) * lax.rsqrt(squares + EPSILON))

    out_copies = {}
    own_copies = {}
    for piece in range(pieces):
        spread = split_dot(jnp.where(in_tensor(piece), factor, 0.0))
        scaled = average[part(piece)] * spread
        moved = MU_OUTER * momentum[part(piece)] + scaled
        new_momentum[part(piece)] = moved
        mine = block_rows(rep, piece)
        full[mine] = params[part(piece)] - LR_OUTER * (scaled + MU_OUTER * moved)
        for step in range(1, chips):
            copy = pltpu.make_async_remote_copy(
                src_ref=full.at[mine],
                dst_ref=full.at[mine],
                send_sem=out_send.at[step - 1, piece],
                recv_sem=out_recv.at[step - 1, piece],
                device_id=(2 * chip_at(step) + core, shard),
                device_id_type=MESH,
            )
            copy.start()
            out_copies[step, piece] = copy
        copy = pltpu.make_async_remote_copy(
            src_ref=full.at[mine],
            dst_ref=full.at[mine],
            send_sem=own_send.at[piece],
            recv_sem=own_recv.at[piece],
            device_id=(twin, shard),
            device_id_type=MESH,
        )
        copy.start()
        own_copies[piece] = copy

    pass_copies = []
    for piece in range(pieces):
        for step in range(1, chips):
            sender = 2 * chip_at(chips - step) + core
            out_copies[step, piece].wait_recv()
            copy = pltpu.make_async_remote_copy(
                src_ref=full.at[block_rows(sender, piece)],
                dst_ref=full.at[block_rows(sender, piece)],
                send_sem=pass_send.at[step - 1, piece],
                recv_sem=pass_recv.at[step - 1, piece],
                device_id=(twin, shard),
                device_id_type=MESH,
            )
            copy.start()
            pass_copies.append(copy)

    for copy in twin_copies.values():
        copy.wait_send()
    for copy in chip_copies.values():
        copy.wait_send()
    pltpu.make_async_copy(partials, partials, norm_send).wait()
    for copy in out_copies.values():
        copy.wait_send()
    for copy in own_copies.values():
        copy.wait()
    for copy in pass_copies:
        copy.wait()


def on_device(replicas, shards, outer_delta, offsets, parameters, momentum):
    rows = parameters.shape[0] // LANES
    block = rows // replicas
    chips = replicas // 2
    chunk = min(block, 128)
    pieces = block // chunk
    devices = replicas * shards
    hbm = pl.BlockSpec(memory_space=pl.ANY)
    vmem = pl.BlockSpec(memory_space=pltpu.VMEM)
    dma = pltpu.SemaphoreType.DMA
    f32 = jnp.float32
    full, moved = pl.pallas_call(
        functools.partial(
            outer_step, replicas, shards, offsets.shape[0] - 1, block, chunk
        ),
        out_shape=(
            jax.ShapeDtypeStruct((rows, LANES), f32),
            jax.ShapeDtypeStruct((block, LANES), f32),
        ),
        in_specs=[pl.BlockSpec(memory_space=pltpu.SMEM), hbm, hbm, hbm],
        out_specs=(vmem, vmem),
        scratch_shapes=[
            pltpu.VMEM((rows, LANES), f32),
            pltpu.VMEM((block, LANES), f32),
            pltpu.VMEM((block, LANES), f32),
            pltpu.VMEM((chips, block, LANES), f32),
            pltpu.VMEM((chips - 1, block, LANES), f32),
            pltpu.VMEM((chips - 1, block, LANES), f32),
            pltpu.VMEM((block, LANES), f32),
            pltpu.VMEM((1, LANES), f32),
            pltpu.VMEM((devices - 1, LANES), f32),
            dma((3,)),
            dma((chips, pieces)),
            dma((chips, pieces)),
            dma((chips - 1, pieces)),
            dma((chips - 1, pieces)),
            dma,
            dma,
            dma((chips - 1, pieces)),
            dma((chips - 1, pieces)),
            dma((pieces,)),
            dma((pieces,)),
            dma((chips - 1, pieces)),
            dma((chips - 1, pieces)),
        ],
        compiler_params=pltpu.CompilerParams(collective_id=0, has_side_effects=True),
        name="outer_step",
    )(
        offsets,
        outer_delta.reshape(rows, LANES),
        parameters.reshape(rows, LANES),
        momentum.reshape(block, LANES),
    )
    return full.reshape(rows * LANES), moved.reshape(block * LANES)


def solution(mesh):
    return jax.shard_map(
        functools.partial(on_device, mesh.shape["rep"], mesh.shape["shard"]),
        mesh=mesh,
        in_specs=(P("rep", "shard"), P(), P("shard"), P(("shard", "rep"))),
        out_specs=(P("shard"), P(("shard", "rep"))),
        check_vma=False,
    )
```

```python
import functools

import jax
import jax.numpy as jnp
from jax import lax
from jax.experimental import pallas as pl
from jax.experimental.pallas import tpu as pltpu
from jax.sharding import PartitionSpec as P

LR_OUTER = 0.7
MU_OUTER = 0.9
CLIP_RMS = 0.1
EPSILON = 1e-06
LANES = 128
MESH = pl.DeviceIdType.MESH


def split_dot(wide):
    high = wide.astype(jnp.bfloat16)
    low = (wide - high.astype(jnp.float32)).astype(jnp.bfloat16)
    both = jnp.concatenate([high, low], axis=1)
    ones = jnp.ones((2 * LANES, LANES), jnp.bfloat16)
    return jnp.dot(both, ones, preferred_element_type=jnp.float32)


def outer_step(
    replicas, shards, tensors, block, chunk,
    offsets, delta_in, params_in, momentum_in,
    full, new_momentum,
    delta, params, momentum, from_twin, chip_sum, from_chips, average, partial, partials,
    load_sem, twin_send, twin_recv, chip_send, chip_recv, norm_send, norm_recv,
    out_send, out_recv, own_send, own_recv, pass_send, pass_recv,
):
    chips = replicas // 2
    pieces = block // chunk
    devices = replicas * shards
    rep = lax.axis_index("rep")
    shard = lax.axis_index("shard")
    me = rep * shards + shard
    chip = lax.div(rep, 2)
    core = lax.rem(rep, 2)
    twin = (rep + 1) - 2 * core

    def chip_at(step):
        return lax.rem(chip + step, chips)

    def part(piece):
        return pl.ds(piece * chunk, chunk)

    own_rows = pl.ds(pl.multiple_of(rep * block, 8), block)
    loads = [
        pltpu.make_async_copy(delta_in, delta, load_sem.at[0]),
        pltpu.make_async_copy(params_in.at[own_rows], params, load_sem.at[1]),
        pltpu.make_async_copy(momentum_in, momentum, load_sem.at[2]),
    ]
    for load in loads:
        load.start()

    barrier = pltpu.get_barrier_semaphore()

    def greet(step, carry):
        other = lax.rem(me + step, devices)
        pl.semaphore_signal(
            barrier, inc=1, device_id=(lax.div(other, shards), lax.rem(other, shards)),
            device_id_type=MESH,
        )
        return carry

    lax.fori_loop(1, devices, greet, 0)

    lane = lax.broadcasted_iota(jnp.int32, (1, LANES), 1)
    first = jnp.zeros((1, LANES), jnp.int32)
    last = jnp.zeros((1, LANES), jnp.int32)
    for t in range(tensors):
        first = jnp.where(lane == t, offsets[t], first)
        last = jnp.where(lane == t, offsets[t + 1], last)

    loads[0].wait()
    pl.semaphore_wait(barrier, devices - 1)

    def block_rows(owner, piece):
        return pl.ds(pl.multiple_of(owner * block + piece * chunk, 8), chunk)

    steps = list(range(1, chips)) + [0]
    twin_copies = {}
    for step in steps:
        for piece in range(pieces):
            owner = 2 * chip_at(step) + (1 - core)
            copy = pltpu.make_async_remote_copy(
                src_ref=delta.at[block_rows(owner, piece)],
                dst_ref=from_twin.at[step, part(piece)],
                send_sem=twin_send.at[step, piece],
                recv_sem=twin_recv.at[step, piece],
                device_id=(twin, shard),
                device_id_type=MESH,
            )
            copy.start()
            twin_copies[step, piece] = copy

    chip_copies = {}
    for piece in range(pieces):
        for step in range(1, chips):
            owner = 2 * chip_at(step) + core
            twin_copies[step, piece].wait_recv()
            chip_sum[step - 1, part(piece)] = (
                delta[block_rows(owner, piece)] + from_twin[step, part(piece)]
            )
            copy = pltpu.make_async_remote_copy(
                src_ref=chip_sum.at[step - 1, part(piece)],
                dst_ref=from_chips.at[step - 1, part(piece)],
                send_sem=chip_send.at[step - 1, piece],
                recv_sem=chip_recv.at[step - 1, piece],
                device_id=(owner, shard),
                device_id_type=MESH,
            )
            copy.start()
            chip_copies[step, piece] = copy

    base = (shard * replicas + rep) * block

    def in_tensor(piece):
        row = lax.broadcasted_iota(jnp.int32, (chunk, LANES), 0)
        position = (row + (base + piece * chunk)) * LANES
        return (position >= first) & (position < last)

    squares = jnp.zeros((1, LANES), jnp.float32)
    for piece in range(pieces):
        twin_copies[0, piece].wait_recv()
        total = delta[block_rows(rep, piece)] + from_twin[0, part(piece)]
        for step in range(1, chips):
            chip_copies[step, piece].wait_recv()
            total = total + from_chips[step - 1, part(piece)]
        mean = total * jnp.float32(1.0 / replicas)
        average[part(piece)] = mean
        row_sums = split_dot(mean * mean)
        squares = squares + jnp.sum(
            jnp.where(in_tensor(piece), row_sums, 0.0), axis=0, keepdims=True
        )
    partial[...] = squares

    def tell(step, carry):
        other = lax.rem(me + step, devices)
        pltpu.make_async_remote_copy(
            src_ref=partial,
            dst_ref=partials.at[pl.ds(step - 1, 1)],
            send_sem=norm_send,
            recv_sem=norm_recv,
            device_id=(lax.div(other, shards), lax.rem(other, shards)),
            device_id_type=MESH,
        ).start()
        return carry

    lax.fori_loop(1, devices, tell, 0)
    loads[1].wait()
    loads[2].wait()
    pltpu.make_async_copy(partials, partials, norm_recv).wait()
    squares = squares + jnp.sum(partials[...], axis=0, keepdims=True)
    lengths = (last - first).astype(jnp.float32)
    factor = jnp.minimum(1.0, CLIP_RMS * jnp.sqrt(lengths) * lax.rsqrt(squares + EPSILON))

    out_copies = {}
    own_copies = {}
    for piece in range(pieces):
        spread = split_dot(jnp.where(in_tensor(piece), factor, 0.0))
        scaled = average[part(piece)] * spread
        moved = MU_OUTER * momentum[part(piece)] + scaled
        new_momentum[part(piece)] = moved
        mine = block_rows(rep, piece)
        full[mine] = params[part(piece)] - LR_OUTER * (scaled + MU_OUTER * moved)
        for step in range(1, chips):
            copy = pltpu.make_async_remote_copy(
                src_ref=full.at[mine],
                dst_ref=full.at[mine],
                send_sem=out_send.at[step - 1, piece],
                recv_sem=out_recv.at[step - 1, piece],
                device_id=(2 * chip_at(step) + core, shard),
                device_id_type=MESH,
            )
            copy.start()
            out_copies[step, piece] = copy
        copy = pltpu.make_async_remote_copy(
            src_ref=full.at[mine],
            dst_ref=full.at[mine],
            send_sem=own_send.at[piece],
            recv_sem=own_recv.at[piece],
            device_id=(twin, shard),
            device_id_type=MESH,
        )
        copy.start()
        own_copies[piece] = copy

    pass_copies = []
    for piece in range(pieces):
        for step in range(1, chips):
            sender = 2 * chip_at(chips - step) + core
            out_copies[step, piece].wait_recv()
            copy = pltpu.make_async_remote_copy(
                src_ref=full.at[block_rows(sender, piece)],
                dst_ref=full.at[block_rows(sender, piece)],
                send_sem=pass_send.at[step - 1, piece],
                recv_sem=pass_recv.at[step - 1, piece],
                device_id=(twin, shard),
                device_id_type=MESH,
            )
            copy.start()
            pass_copies.append(copy)

    for copy in twin_copies.values():
        copy.wait_send()
    for copy in chip_copies.values():
        copy.wait_send()
    pltpu.make_async_copy(partials, partials, norm_send).wait()
    for copy in out_copies.values():
        copy.wait_send()
    for copy in own_copies.values():
        copy.wait()
    for copy in pass_copies:
        copy.wait()


def put_out(full, moved, full_out, moved_out, sem):
    copies = [
        pltpu.make_async_copy(full, full_out, sem.at[0]),
        pltpu.make_async_copy(moved, moved_out, sem.at[1]),
    ]
    for copy in copies:
        copy.start()
    for copy in copies:
        copy.wait()


def on_device(replicas, shards, outer_delta, offsets, parameters, momentum):
    rows = parameters.shape[0] // LANES
    block = rows // replicas
    chips = replicas // 2
    chunk = min(block, 128)
    pieces = block // chunk
    devices = replicas * shards
    hbm = pl.BlockSpec(memory_space=pltpu.HBM)
    vmem = pl.BlockSpec(memory_space=pltpu.VMEM)
    dma = pltpu.SemaphoreType.DMA
    f32 = jnp.float32
    full, moved = pl.pallas_call(
        functools.partial(
            outer_step, replicas, shards, offsets.shape[0] - 1, block, chunk
        ),
        out_shape=(
            jax.ShapeDtypeStruct((rows, LANES), f32),
            jax.ShapeDtypeStruct((block, LANES), f32),
        ),
        in_specs=[pl.BlockSpec(memory_space=pltpu.SMEM), hbm, hbm, hbm],
        out_specs=(vmem, vmem),
        scratch_shapes=[
            pltpu.VMEM((rows, LANES), f32),
            pltpu.VMEM((block, LANES), f32),
            pltpu.VMEM((block, LANES), f32),
            pltpu.VMEM((chips, block, LANES), f32),
            pltpu.VMEM((chips - 1, block, LANES), f32),
            pltpu.VMEM((chips - 1, block, LANES), f32),
            pltpu.VMEM((block, LANES), f32),
            pltpu.VMEM((1, LANES), f32),
            pltpu.VMEM((devices - 1, LANES), f32),
            dma((3,)),
            dma((chips, pieces)),
            dma((chips, pieces)),
            dma((chips - 1, pieces)),
            dma((chips - 1, pieces)),
            dma,
            dma,
            dma((chips - 1, pieces)),
            dma((chips - 1, pieces)),
            dma((pieces,)),
            dma((pieces,)),
            dma((chips - 1, pieces)),
            dma((chips - 1, pieces)),
        ],
        compiler_params=pltpu.CompilerParams(collective_id=0, has_side_effects=True, vmem_limit_bytes=12 * 2**20),
        name="outer_step",
    )(
        pltpu.with_memory_space_constraint(offsets, pltpu.HBM),
        pltpu.with_memory_space_constraint(outer_delta.reshape(rows, LANES), pltpu.HBM),
        pltpu.with_memory_space_constraint(parameters.reshape(rows, LANES), pltpu.HBM),
        pltpu.with_memory_space_constraint(momentum.reshape(block, LANES), pltpu.HBM),
    )
    full, moved = pl.pallas_call(
        put_out,
        out_shape=(
            jax.ShapeDtypeStruct((rows, LANES), f32),
            jax.ShapeDtypeStruct((block, LANES), f32),
        ),
        in_specs=[pl.BlockSpec(memory_space=pl.ANY)] * 2,
        out_specs=(hbm, hbm),
        scratch_shapes=[dma((2,))],
        compiler_params=pltpu.CompilerParams(vmem_limit_bytes=2**20),
        name="put_out",
    )(full, moved)
    return full.reshape(rows * LANES), moved.reshape(block * LANES)


def solution(mesh):
    return jax.shard_map(
        functools.partial(on_device, mesh.shape["rep"], mesh.shape["shard"]),
        mesh=mesh,
        in_specs=(P("rep", "shard"), P(), P("shard"), P(("shard", "rep"))),
        out_specs=(P("shard"), P(("shard", "rep"))),
        check_vma=False,
    )
```

```python
import functools

import jax
import jax.numpy as jnp
from jax import lax
from jax.experimental import pallas as pl
from jax.experimental.pallas import tpu as pltpu
from jax.sharding import PartitionSpec as P

LR_OUTER = 0.7
MU_OUTER = 0.9
CLIP_RMS = 0.1
EPSILON = 1e-06
LANES = 128
MESH = pl.DeviceIdType.MESH


def split_dot(wide):
    high = wide.astype(jnp.bfloat16)
    low = (wide - high.astype(jnp.float32)).astype(jnp.bfloat16)
    both = jnp.concatenate([high, low], axis=1)
    ones = jnp.ones((2 * LANES, LANES), jnp.bfloat16)
    return jnp.dot(both, ones, preferred_element_type=jnp.float32)


def outer_step(
    replicas, shards, tensors, block, chunk, early, ahead, before,
    offsets, delta_in, params_in, momentum_in,
    full, new_momentum,
    delta, params, momentum, average, from_twin, chip_sum, from_chips, partial, partials,
    ready, everyone, load_sem, twin_send, twin_recv, chip_send, chip_recv, norm_send, norm_recv,
    out_send, out_recv, own_send, own_recv, pass_send, pass_recv,
):
    chips = replicas // 2
    pieces = block // chunk
    devices = replicas * shards
    rep = lax.axis_index("rep")
    shard = lax.axis_index("shard")
    me = rep * shards + shard
    chip = lax.div(rep, 2)
    core = lax.rem(rep, 2)
    twin = (rep + 1) - 2 * core
    peers = range(1, chips)

    def peer(step):
        return 2 * lax.rem(chip + step, chips) + core

    def part(piece):
        return pl.ds(piece * chunk, chunk)

    def block_rows(owner, piece):
        return pl.ds(pl.multiple_of(owner * block + piece * chunk, 8), chunk)

    def to(other, src, dst, send, recv):
        copy = pltpu.make_async_remote_copy(
            src_ref=src, dst_ref=dst, send_sem=send, recv_sem=recv,
            device_id=(other, shard), device_id_type=MESH,
        )
        copy.start()
        return copy

    own_rows = pl.ds(pl.multiple_of(rep * block, 8), block)
    loads = [
        pltpu.make_async_copy(momentum_in, momentum.at[own_rows], load_sem.at[0]),
        pltpu.make_async_copy(delta_in, delta, load_sem.at[1]),
        pltpu.make_async_copy(params_in, params, load_sem.at[2]),
    ]
    for load in loads:
        load.start()

    barrier = pltpu.get_barrier_semaphore()

    @pl.when(rep != 0)
    def _():
        for step in range(1, replicas):
            other = lax.rem(rep + step, replicas)

            @pl.when(other != 0)
            def _():
                pl.semaphore_signal(
                    barrier, inc=1, device_id=(other, shard), device_id_type=MESH
                )

        pl.semaphore_wait(barrier, replicas - 1)
        pl.semaphore_signal(ready, inc=1, device_id=(0, shard), device_id_type=MESH)

    @pl.when(rep == 0)
    def _():
        for other in range(1, replicas):
            pl.semaphore_signal(
                barrier, inc=1, device_id=(other, shard), device_id_type=MESH
            )
        pl.semaphore_wait(ready, replicas - 1)
        for step in range(1, shards):
            pl.semaphore_signal(
                barrier, inc=1, device_id=(rep, lax.rem(shard + step, shards)),
                device_id_type=MESH,
            )

    lane = lax.broadcasted_iota(jnp.int32, (1, LANES), 1)
    first = jnp.zeros((1, LANES), jnp.int32)
    last = jnp.zeros((1, LANES), jnp.int32)
    for t in range(tensors):
        first = jnp.where(lane == t, offsets[t], first)
        last = jnp.where(lane == t, offsets[t + 1], last)

    def in_tensor(owner, piece):
        row = lax.broadcasted_iota(jnp.int32, (chunk, LANES), 0)
        start = (shard * replicas + owner) * block + piece * chunk
        position = (row + start) * LANES
        return (position >= first) & (position < last)

    arrays = (momentum, average, full)
    sent = {}
    own = {}
    passed = []

    def share(kind, piece):
        mine = arrays[kind].at[block_rows(rep, piece)]
        for step in peers:
            sent[kind, step, piece] = to(
                peer(step), mine, mine,
                out_send.at[kind, step - 1, piece], out_recv.at[kind, step - 1, piece],
            )
        own[kind, piece] = to(
            twin, mine, mine, own_send.at[kind, piece], own_recv.at[kind, piece]
        )

    def pass_on(kind, piece):
        for step in peers:
            sent[kind, step, piece].wait_recv()
            rows = arrays[kind].at[block_rows(peer(chips - step), piece)]
            passed.append((kind, piece, to(
                twin, rows, rows,
                pass_send.at[kind, step - 1, piece], pass_recv.at[kind, step - 1, piece],
            )))

    loads[0].wait()
    loads[1].wait()

    twin_copies = {}
    for step in list(peers) + [0]:
        for piece in range(pieces):
            owner = peer(step) + 1 - 2 * core
            twin_copies[step, piece] = to(
                twin, delta.at[block_rows(owner, piece)], from_twin.at[step, part(piece)],
                twin_send.at[step, piece], twin_recv.at[step, piece],
            )
        if step == (1 if chips > 1 else 0):
            for piece in range(ahead):
                share(0, piece)

    chip_copies = {}
    for piece in range(pieces):
        for step in peers:
            twin_copies[step, piece].wait_recv()
            chip_sum[step - 1, part(piece)] = (
                delta[block_rows(peer(step), piece)] + from_twin[step, part(piece)]
            )
            chip_copies[step, piece] = to(
                peer(step), chip_sum.at[step - 1, part(piece)],
                from_chips.at[step - 1, part(piece)],
                chip_send.at[step - 1, piece], chip_recv.at[step - 1, piece],
            )
    if ahead < early:
        share(0, ahead)

    @pl.when(rep == 0)
    def _():
        pl.semaphore_wait(barrier, shards - 1)
        for other in range(1, replicas):
            pl.semaphore_signal(
                everyone, inc=1, device_id=(other, shard), device_id_type=MESH
            )

    squares = jnp.zeros((1, LANES), jnp.float32)
    for piece in range(pieces):
        twin_copies[0, piece].wait_recv()
        total = delta[block_rows(rep, piece)] + from_twin[0, part(piece)]
        for step in peers:
            chip_copies[step, piece].wait_recv()
            total = total + from_chips[step - 1, part(piece)]
        mean = total * jnp.float32(1.0 / replicas)
        average[block_rows(rep, piece)] = mean
        row_sums = split_dot(mean * mean)
        squares = squares + jnp.sum(
            jnp.where(in_tensor(rep, piece), row_sums, 0.0), axis=0, keepdims=True
        )
    partial[...] = squares

    @pl.when(rep != 0)
    def _():
        pl.semaphore_wait(everyone, 1)

    def tell(step, carry):
        other = lax.rem(me + step, devices)
        pltpu.make_async_remote_copy(
            src_ref=partial,
            dst_ref=partials.at[pl.ds(step - 1, 1)],
            send_sem=norm_send,
            recv_sem=norm_recv,
            device_id=(lax.div(other, shards), lax.rem(other, shards)),
            device_id_type=MESH,
        ).start()
        return carry

    lax.fori_loop(1, devices, tell, 0)

    queue = []
    for piece in range(early):
        share(1, piece)
        if (0, piece) not in own:
            share(0, piece)
        queue.append((1, piece))
        queue.append((0, piece))
    queue.sort(key=lambda item: not (item[0] == 0 and item[1] <= ahead))
    for kind, piece in queue[:before]:
        pass_on(kind, piece)

    loads[2].wait()
    pltpu.make_async_copy(partials, partials, norm_recv).wait()
    squares = squares + jnp.sum(partials[...], axis=0, keepdims=True)
    lengths = (last - first).astype(jnp.float32)
    factor = jnp.minimum(1.0, CLIP_RMS * jnp.sqrt(lengths) * lax.rsqrt(squares + EPSILON))

    def update(owner, piece):
        rows = block_rows(owner, piece)
        spread = split_dot(jnp.where(in_tensor(owner, piece), factor, 0.0))
        scaled = average[rows] * spread
        moved = MU_OUTER * momentum[rows] + scaled
        full[rows] = params[rows] - LR_OUTER * (scaled + MU_OUTER * moved)
        return moved

    for piece in range(early, pieces):
        new_momentum[part(piece)] = update(rep, piece)
        share(2, piece)
    for kind, piece in queue[before:]:
        pass_on(kind, piece)
    for piece in range(early):
        new_momentum[part(piece)] = update(rep, piece)
    for piece in range(early):
        own[0, piece].wait_recv()
        own[1, piece].wait_recv()
        update(twin, piece)
    for piece in range(early):
        for step in peers:
            update(peer(step), piece)
    for piece in range(early, pieces):
        pass_on(2, piece)
    for kind, piece, copy in passed:
        if kind < 2:
            copy.wait_recv()
    for piece in range(early):
        for step in peers:
            update(peer(step) + 1 - 2 * core, piece)

    for copy in (*twin_copies.values(), *chip_copies.values(), *sent.values()):
        copy.wait_send()
    pltpu.make_async_copy(partials, partials, norm_send).wait()
    for (kind, piece), copy in own.items():
        copy.wait_send()
        if kind == 2:
            copy.wait_recv()
    for kind, piece, copy in passed:
        copy.wait_send()
        if kind == 2:
            copy.wait_recv()


def put_out(full, moved, full_out, moved_out, sem):
    copies = [
        pltpu.make_async_copy(full, full_out, sem.at[0]),
        pltpu.make_async_copy(moved, moved_out, sem.at[1]),
    ]
    for copy in copies:
        copy.start()
    for copy in copies:
        copy.wait()


def on_device(replicas, shards, outer_delta, offsets, parameters, momentum):
    rows = parameters.shape[0] // LANES
    block = rows // replicas
    chips = replicas // 2
    chunk = min(block, 128)
    pieces = block // chunk
    early = pieces * 3 // 4
    ahead = min(early, 1)
    before = min(2 * early, 2)
    devices = replicas * shards
    hbm = pl.BlockSpec(memory_space=pltpu.HBM)
    vmem = pl.BlockSpec(memory_space=pltpu.VMEM)
    dma = pltpu.SemaphoreType.DMA
    f32 = jnp.float32
    full, moved = pl.pallas_call(
        functools.partial(
            outer_step, replicas, shards, offsets.shape[0] - 1, block, chunk,
            early, ahead, before,
        ),
        out_shape=(
            jax.ShapeDtypeStruct((rows, LANES), f32),
            jax.ShapeDtypeStruct((block, LANES), f32),
        ),
        in_specs=[pl.BlockSpec(memory_space=pltpu.SMEM), hbm, hbm, hbm],
        out_specs=(vmem, vmem),
        scratch_shapes=[
            pltpu.VMEM((rows, LANES), f32),
            pltpu.VMEM((rows, LANES), f32),
            pltpu.VMEM((rows, LANES), f32),
            pltpu.VMEM((rows, LANES), f32),
            pltpu.VMEM((chips, block, LANES), f32),
            pltpu.VMEM((chips - 1, block, LANES), f32),
            pltpu.VMEM((chips - 1, block, LANES), f32),
            pltpu.VMEM((1, LANES), f32),
            pltpu.VMEM((devices - 1, LANES), f32),
            pltpu.SemaphoreType.REGULAR,
            pltpu.SemaphoreType.REGULAR,
            dma((3,)),
            dma((chips, pieces)),
            dma((chips, pieces)),
            dma((chips - 1, pieces)),
            dma((chips - 1, pieces)),
            dma,
            dma,
            dma((3, chips - 1, pieces)),
            dma((3, chips - 1, pieces)),
            dma((3, pieces)),
            dma((3, pieces)),
            dma((3, chips - 1, pieces)),
            dma((3, chips - 1, pieces)),
        ],
        compiler_params=pltpu.CompilerParams(collective_id=0, has_side_effects=True, vmem_limit_bytes=12 * 2**20),
        name="outer_step",
    )(
        pltpu.with_memory_space_constraint(offsets, pltpu.HBM),
        pltpu.with_memory_space_constraint(outer_delta.reshape(rows, LANES), pltpu.HBM),
        pltpu.with_memory_space_constraint(parameters.reshape(rows, LANES), pltpu.HBM),
        pltpu.with_memory_space_constraint(momentum.reshape(block, LANES), pltpu.HBM),
    )
    full, moved = pl.pallas_call(
        put_out,
        out_shape=(
            jax.ShapeDtypeStruct((rows, LANES), f32),
            jax.ShapeDtypeStruct((block, LANES), f32),
        ),
        in_specs=[pl.BlockSpec(memory_space=pl.ANY)] * 2,
        out_specs=(hbm, hbm),
        scratch_shapes=[dma((2,))],
        compiler_params=pltpu.CompilerParams(vmem_limit_bytes=2**20),
        name="put_out",
    )(full, moved)
    return full.reshape(rows * LANES), moved.reshape(block * LANES)


def solution(mesh):
    return jax.shard_map(
        functools.partial(on_device, mesh.shape["rep"], mesh.shape["shard"]),
        mesh=mesh,
        in_specs=(P("rep", "shard"), P(), P("shard"), P(("shard", "rep"))),
        out_specs=(P("shard"), P(("shard", "rep"))),
        check_vma=False,
    )
```

```python
import functools

import jax
import jax.numpy as jnp
from jax import lax
from jax.experimental import pallas as pl
from jax.experimental.pallas import tpu as pltpu
from jax.sharding import PartitionSpec as P

LR_OUTER = 0.7
MU_OUTER = 0.9
CLIP_RMS = 0.1
EPSILON = 1e-06
LANES = 128
MESH = pl.DeviceIdType.MESH


def split_dot(wide):
    high = wide.astype(jnp.bfloat16)
    low = (wide - high.astype(jnp.float32)).astype(jnp.bfloat16)
    both = jnp.concatenate([high, low], axis=1)
    ones = jnp.ones((2 * LANES, LANES), jnp.bfloat16)
    return jnp.dot(both, ones, preferred_element_type=jnp.float32)


def outer_step(
    replicas, shards, tensors, block, chunk, early, ahead, before,
    offsets, delta_in, params_in, momentum_in,
    full, new_momentum,
    delta, params, momentum, average, from_twin, chip_sum, from_chips, partial, partials,
    ready, everyone, load_sem, twin_send, twin_recv, chip_send, chip_recv, norm_send, norm_recv,
    out_send, out_recv, own_send, own_recv, pass_send, pass_recv,
):
    chips = replicas // 2
    pieces = block // chunk
    devices = replicas * shards
    rep = lax.axis_index("rep")
    shard = lax.axis_index("shard")
    me = rep * shards + shard
    chip = lax.div(rep, 2)
    core = lax.rem(rep, 2)
    twin = (rep + 1) - 2 * core
    peers = range(1, chips)

    def peer(step):
        return 2 * lax.rem(chip + step, chips) + core

    def part(piece):
        return pl.ds(piece * chunk, chunk)

    def block_rows(owner, piece):
        return pl.ds(pl.multiple_of(owner * block + piece * chunk, 8), chunk)

    def to(other, src, dst, send, recv):
        copy = pltpu.make_async_remote_copy(
            src_ref=src, dst_ref=dst, send_sem=send, recv_sem=recv,
            device_id=(other, shard), device_id_type=MESH,
        )
        copy.start()
        return copy

    own_rows = pl.ds(pl.multiple_of(rep * block, 8), block)
    loads = [
        pltpu.make_async_copy(momentum_in, momentum.at[own_rows], load_sem.at[0]),
        pltpu.make_async_copy(delta_in, delta, load_sem.at[1]),
        pltpu.make_async_copy(params_in, params, load_sem.at[2]),
    ]
    for load in loads:
        load.start()

    barrier = pltpu.get_barrier_semaphore()

    @pl.when(rep != 0)
    def _():
        for step in range(1, replicas):
            other = lax.rem(rep + step, replicas)

            @pl.when(other != 0)
            def _():
                pl.semaphore_signal(
                    barrier, inc=1, device_id=(other, shard), device_id_type=MESH
                )

        pl.semaphore_wait(barrier, replicas - 1)
        pl.semaphore_signal(ready, inc=1, device_id=(0, shard), device_id_type=MESH)

    @pl.when(rep == 0)
    def _():
        for other in range(1, replicas):
            pl.semaphore_signal(
                barrier, inc=1, device_id=(other, shard), device_id_type=MESH
            )
        pl.semaphore_wait(ready, replicas - 1)
        for step in range(1, shards):
            pl.semaphore_signal(
                barrier, inc=1, device_id=(rep, lax.rem(shard + step, shards)),
                device_id_type=MESH,
            )

    lane = lax.broadcasted_iota(jnp.int32, (1, LANES), 1)
    first = jnp.zeros((1, LANES), jnp.int32)
    last = jnp.zeros((1, LANES), jnp.int32)
    for t in range(tensors):
        first = jnp.where(lane == t, offsets[t], first)
        last = jnp.where(lane == t, offsets[t + 1], last)

    def in_tensor(owner, piece):
        row = lax.broadcasted_iota(jnp.int32, (chunk, LANES), 0)
        start = (shard * replicas + owner) * block + piece * chunk
        position = (row + start) * LANES
        return (position >= first) & (position < last)

    arrays = (momentum, average, full)
    sent = {}
    own = {}
    passed = []

    def share(kind, piece):
        mine = arrays[kind].at[block_rows(rep, piece)]
        for step in peers:
            sent[kind, step, piece] = to(
                peer(step), mine, mine,
                out_send.at[kind, step - 1, piece], out_recv.at[kind, step - 1, piece],
            )
        if kind == 2:
            own[kind, piece] = to(
                twin, mine, mine, own_send.at[kind, piece], own_recv.at[kind, piece]
            )

    def share_early(kind):
        rows = pl.ds(pl.multiple_of(rep * block, 8), early * chunk)
        mine = arrays[kind].at[rows]
        own[kind, 0] = to(twin, mine, mine, own_send.at[kind, 0], own_recv.at[kind, 0])

    def pass_on(kind, piece):
        for step in peers:
            sent[kind, step, piece].wait_recv()
            rows = arrays[kind].at[block_rows(peer(chips - step), piece)]
            passed.append((kind, piece, to(
                twin, rows, rows,
                pass_send.at[kind, step - 1, piece], pass_recv.at[kind, step - 1, piece],
            )))

    loads[0].wait()
    loads[1].wait()

    twin_copies = {}
    for step in list(peers) + [0]:
        for piece in range(pieces):
            owner = peer(step) + 1 - 2 * core
            twin_copies[step, piece] = to(
                twin, delta.at[block_rows(owner, piece)], from_twin.at[step, part(piece)],
                twin_send.at[step, piece], twin_recv.at[step, piece],
            )
        if step == (1 if chips > 1 else 0):
            for piece in range(ahead):
                share(0, piece)

    chip_copies = {}
    for piece in range(pieces):
        for step in peers:
            twin_copies[step, piece].wait_recv()
            chip_sum[step - 1, part(piece)] = (
                delta[block_rows(peer(step), piece)] + from_twin[step, part(piece)]
            )
            chip_copies[step, piece] = to(
                peer(step), chip_sum.at[step - 1, part(piece)],
                from_chips.at[step - 1, part(piece)],
                chip_send.at[step - 1, piece], chip_recv.at[step - 1, piece],
            )
    if ahead < early:
        share(0, ahead)

    @pl.when(rep == 0)
    def _():
        pl.semaphore_wait(barrier, shards - 1)
        for other in range(1, replicas):
            pl.semaphore_signal(
                everyone, inc=1, device_id=(other, shard), device_id_type=MESH
            )

    squares = jnp.zeros((1, LANES), jnp.float32)
    for piece in range(pieces):
        twin_copies[0, piece].wait_recv()
        total = delta[block_rows(rep, piece)] + from_twin[0, part(piece)]
        for step in peers:
            chip_copies[step, piece].wait_recv()
            total = total + from_chips[step - 1, part(piece)]
        mean = total * jnp.float32(1.0 / replicas)
        average[block_rows(rep, piece)] = mean
        row_sums = split_dot(mean * mean)
        squares = squares + jnp.sum(
            jnp.where(in_tensor(rep, piece), row_sums, 0.0), axis=0, keepdims=True
        )
    partial[...] = squares

    @pl.when(rep != 0)
    def _():
        pl.semaphore_wait(everyone, 1)

    def tell(step, carry):
        other = lax.rem(me + step, devices)
        pltpu.make_async_remote_copy(
            src_ref=partial,
            dst_ref=partials.at[pl.ds(step - 1, 1)],
            send_sem=norm_send,
            recv_sem=norm_recv,
            device_id=(lax.div(other, shards), lax.rem(other, shards)),
            device_id_type=MESH,
        ).start()
        return carry

    lax.fori_loop(1, devices, tell, 0, unroll=devices <= 64)

    queue = []
    for piece in range(early):
        share(1, piece)
        if piece > ahead:
            share(0, piece)
        queue.append((1, piece))
        queue.append((0, piece))
    if early:
        share_early(0)
        share_early(1)
    queue.sort(key=lambda item: not (item[0] == 0 and item[1] <= ahead))
    for kind, piece in queue[:before]:
        pass_on(kind, piece)

    loads[2].wait()
    pltpu.make_async_copy(partials, partials, norm_recv).wait()
    squares = squares + jnp.sum(partials[...], axis=0, keepdims=True)
    lengths = (last - first).astype(jnp.float32)
    factor = jnp.minimum(1.0, CLIP_RMS * jnp.sqrt(lengths) * lax.rsqrt(squares + EPSILON))

    def update(owner, piece):
        rows = block_rows(owner, piece)
        spread = split_dot(jnp.where(in_tensor(owner, piece), factor, 0.0))
        scaled = average[rows] * spread
        moved = MU_OUTER * momentum[rows] + scaled
        full[rows] = params[rows] - LR_OUTER * (scaled + MU_OUTER * moved)
        return moved

    for piece in range(early, pieces):
        new_momentum[part(piece)] = update(rep, piece)
        share(2, piece)
    for kind, piece in queue[before:]:
        pass_on(kind, piece)
    for piece in range(early):
        new_momentum[part(piece)] = update(rep, piece)
    if early:
        own[0, 0].wait_recv()
        own[1, 0].wait_recv()
    for piece in range(early):
        update(twin, piece)
    for piece in range(early):
        for step in peers:
            update(peer(step), piece)
    for piece in range(early, pieces):
        pass_on(2, piece)
    for kind, piece, copy in passed:
        if kind < 2:
            copy.wait_recv()
    for piece in range(early):
        for step in peers:
            update(peer(step) + 1 - 2 * core, piece)

    for copy in (*twin_copies.values(), *chip_copies.values(), *sent.values()):
        copy.wait_send()
    pltpu.make_async_copy(partials, partials, norm_send).wait()
    for (kind, piece), copy in own.items():
        copy.wait_send()
        if kind == 2:
            copy.wait_recv()
    for kind, piece, copy in passed:
        copy.wait_send()
        if kind == 2:
            copy.wait_recv()


def put_out(full, moved, full_out, moved_out, sem):
    copies = [
        pltpu.make_async_copy(full, full_out, sem.at[0]),
        pltpu.make_async_copy(moved, moved_out, sem.at[1]),
    ]
    for copy in copies:
        copy.start()
    for copy in copies:
        copy.wait()


def on_device(replicas, shards, outer_delta, offsets, parameters, momentum):
    rows = parameters.shape[0] // LANES
    block = rows // replicas
    chips = replicas // 2
    chunk = min(block, 128)
    pieces = block // chunk
    early = pieces * 3 // 4
    ahead = min(early, 1)
    before = min(2 * early, 2)
    devices = replicas * shards
    hbm = pl.BlockSpec(memory_space=pltpu.HBM)
    vmem = pl.BlockSpec(memory_space=pltpu.VMEM)
    dma = pltpu.SemaphoreType.DMA
    f32 = jnp.float32
    full, moved = pl.pallas_call(
        functools.partial(
            outer_step, replicas, shards, offsets.shape[0] - 1, block, chunk,
            early, ahead, before,
        ),
        out_shape=(
            jax.ShapeDtypeStruct((rows, LANES), f32),
            jax.ShapeDtypeStruct((block, LANES), f32),
        ),
        in_specs=[pl.BlockSpec(memory_space=pltpu.SMEM), hbm, hbm, hbm],
        out_specs=(vmem, vmem),
        scratch_shapes=[
            pltpu.VMEM((rows, LANES), f32),
            pltpu.VMEM((rows, LANES), f32),
            pltpu.VMEM((rows, LANES), f32),
            pltpu.VMEM((rows, LANES), f32),
            pltpu.VMEM((chips, block, LANES), f32),
            pltpu.VMEM((chips - 1, block, LANES), f32),
            pltpu.VMEM((chips - 1, block, LANES), f32),
            pltpu.VMEM((1, LANES), f32),
            pltpu.VMEM((devices - 1, LANES), f32),
            pltpu.SemaphoreType.REGULAR,
            pltpu.SemaphoreType.REGULAR,
            dma((3,)),
            dma((chips, pieces)),
            dma((chips, pieces)),
            dma((chips - 1, pieces)),
            dma((chips - 1, pieces)),
            dma,
            dma,
            dma((3, chips - 1, pieces)),
            dma((3, chips - 1, pieces)),
            dma((3, pieces)),
            dma((3, pieces)),
            dma((3, chips - 1, pieces)),
            dma((3, chips - 1, pieces)),
        ],
        compiler_params=pltpu.CompilerParams(collective_id=0, has_side_effects=True, vmem_limit_bytes=12 * 2**20),
        name="outer_step",
    )(
        pltpu.with_memory_space_constraint(offsets, pltpu.HBM),
        pltpu.with_memory_space_constraint(outer_delta.reshape(rows, LANES), pltpu.HBM),
        pltpu.with_memory_space_constraint(parameters.reshape(rows, LANES), pltpu.HBM),
        pltpu.with_memory_space_constraint(momentum.reshape(block, LANES), pltpu.HBM),
    )
    full, moved = pl.pallas_call(
        put_out,
        out_shape=(
            jax.ShapeDtypeStruct((rows, LANES), f32),
            jax.ShapeDtypeStruct((block, LANES), f32),
        ),
        in_specs=[pl.BlockSpec(memory_space=pl.ANY)] * 2,
        out_specs=(hbm, hbm),
        scratch_shapes=[dma((2,))],
        compiler_params=pltpu.CompilerParams(vmem_limit_bytes=2**20),
        name="put_out",
    )(full, moved)
    return full.reshape(rows * LANES), moved.reshape(block * LANES)


def solution(mesh):
    return jax.shard_map(
        functools.partial(on_device, mesh.shape["rep"], mesh.shape["shard"]),
        mesh=mesh,
        in_specs=(P("rep", "shard"), P(), P("shard"), P(("shard", "rep"))),
        out_specs=(P("shard"), P(("shard", "rep"))),
        check_vma=False,
    )
```
